32 devices in a mesh: ep: 8 (over y, x, core), dp: 4 (over z).
Axes of the slice: x: 2, y: 2, z: 4, core: 2. Of those that a mesh axis runs over, the one named last changes fastest.
Arguments:
- master_weights: float32 [8, 1024, 3584], P('ep', 'dp'), may hold values from -6 to 6
- first_moment: float32 [8, 1024, 3584], P('ep', 'dp'), may hold values from -6 to 6
- second_moment: float32 [8, 1024, 3584], P('ep', 'dp'), may hold values from 0.01 to 4
- expert_ids: int32 [8], replicated, may hold values from 0 to 255, as said below
- bucket_offsets: int32 [1024], replicated, may hold values from 0 to 1023, as said below
- writer_rank: int32 [1024], replicated, may hold values from 0 to 3, as said below
Outputs:
- saved: bfloat16 [3, 8, 1024, 3584], P(None, 'ep', 'dp')
The draws below stay inside these ranges and needn't reach their ends.
Inputs may be any that keep to these rules, and one draw needn't show every extreme that they name: `expert_ids`: 8 different global expert numbers. `bucket_offsets`: each saved row named exactly once. `writer_rank`: of the bucket rows held by any one dp index, exactly 1024 // (4 * 4) are written by each dp index.
All inputs are finite; a program needn't handle non-finite values.
Results may differ from the reference program's by a relative error of at most 0.001.
Values may be sent and summed in bfloat16 or wider, within the bound.
No kernel may reach another device: no remote copies, remote signals or barrier semaphores. Data moves between devices by JAX's collectives and lax.ppermute only.
A program may use at most 128 MiB of HBM per device.

```python
import math
import jax
import jax.numpy as jnp

ROWS = 1024
COLS = 3584
ALL_EXPERTS = 256
EXPERTS = 8
N_DP = 4


def layout_tables(key):
    shard_rows = ROWS // N_DP
    shuffle = jax.random.permutation(jax.random.fold_in(key, 11), ROWS).astype(jnp.int32)
    pattern = jnp.tile(jnp.arange(N_DP, dtype=jnp.int32), shard_rows // N_DP)
    shard_keys = jax.random.split(jax.random.fold_in(key, 12), N_DP)
    chosen = jax.vmap(lambda single: jax.random.permutation(single, pattern))(shard_keys).reshape(ROWS)
    writers = jnp.zeros((ROWS,), jnp.int32).at[shuffle].set(chosen.astype(jnp.int32))
    return (shuffle, writers)


def draw_expert_ids(key, part):
    return jax.random.permutation(jax.random.fold_in(key, 5), ALL_EXPERTS)[:EXPERTS].astype(jnp.int32)


def draw_bucket_offsets(key, part):
    return layout_tables(key)[0]


def draw_writer_rank(key, part):
    return layout_tables(key)[1]


def level_of(key, dims, cuts, least, high):
    level = 1.0
    for dim, parts in cuts:
        draws = jax.random.uniform(jax.random.fold_in(jax.random.fold_in(key, 6), dim), (parts,), jnp.float32, least / len(cuts), high / len(cuts))
        level = level * jnp.repeat(jnp.exp(draws), dims[dim] // parts).reshape((-1,) + (1,) * (len(dims) - 1 - dim))
    return level


def scatter_about(own_key, dims, spread, limit, shards=(), kind=jnp.bfloat16):
    drawn = spread * jax.random.normal(own_key, dims, jnp.float32)
    if shards:
        drawn = drawn * level_of(own_key, dims, shards, -0.22, 0.18)
    return jnp.clip(drawn, -limit, limit).astype(kind)


def setup_inputs(seed: int = 0) -> dict:
    streams_of = jax.random.split(jax.random.key(seed), 7)
    master_weights = scatter_about(streams_of[0], (EXPERTS, ROWS, COLS), 1.0, 6.0, ((0, 8), (1, 4)), jnp.float32)
    first_moment = scatter_about(streams_of[1], (EXPERTS, ROWS, COLS), 1.0, 6.0, ((0, 8), (1, 4)), jnp.float32)
    second_moment = jnp.clip(jnp.exp(math.log(4.0) - 5.9914646 * jax.random.uniform(streams_of[2], (EXPERTS, ROWS, COLS), jnp.float32) ** level_of(streams_of[2], (EXPERTS, ROWS, COLS), ((0, 8), (1, 4)), -0.2, 0.2)), 0.01, 4.0)
    expert_ids = draw_expert_ids(jax.random.fold_in(streams_of[6], 71), 0)
    bucket_offsets = draw_bucket_offsets(jax.random.fold_in(streams_of[6], 71), 0)
    writer_rank = draw_writer_rank(jax.random.fold_in(streams_of[6], 71), 0)
    return {"master_weights": master_weights, "first_moment": first_moment, "second_moment": second_moment, "expert_ids": expert_ids, "bucket_offsets": bucket_offsets, "writer_rank": writer_rank}


def destinations(bucket_offsets, writer_rank, shard_rows, groups):
    indicator = (writer_rank[:, None] == jnp.arange(groups, dtype=jnp.int32)[None, :]).astype(jnp.int32)
    before = jnp.cumsum(indicator, axis=0) - indicator
    within = jnp.sum(before * indicator, axis=1).astype(jnp.int32)
    placed = writer_rank * shard_rows + within
    return jnp.take(placed, bucket_offsets)


def reference(master_weights, first_moment, second_moment, expert_ids, bucket_offsets, writer_rank):
    target = destinations(bucket_offsets, writer_rank, ROWS // N_DP, N_DP)
    source_rows = jnp.argsort(target)
    source_order = jnp.argsort(expert_ids)

    def arrange(field):
        moved = jnp.take(field.astype(jnp.bfloat16), source_order, axis=0)
        return jnp.take(moved, source_rows, axis=1)

    return jnp.stack([arrange(master_weights), arrange(first_moment), arrange(second_moment)])
```

```python
import functools

import jax
import jax.numpy as jnp
from jax import lax
from jax.experimental import pallas as pl
from jax.experimental.pallas import tpu as pltpu
from jax.sharding import PartitionSpec as P


FIELDS = 3
LANES = 128
ANY = pl.BlockSpec(memory_space=pl.ANY)
SMEM = pl.BlockSpec(memory_space=pltpu.SMEM)
VMEM = pl.BlockSpec(memory_space=pltpu.VMEM)
NT = (((1,), (1,)), ((), ()))


def iota(shape, dim):
    return lax.broadcasted_iota(jnp.int32, shape, dim)


def ones_where(mask):
    return jnp.where(mask, 1.0, 0.0).astype(jnp.bfloat16)


def dot(a, b):
    return jnp.dot(a, b, preferred_element_type=jnp.float32)


def plan_kernel(groups, dp_ref, offsets_ref, writer_ref, send_ref, place_ref):
    rows = offsets_ref.shape[1]
    shard = rows // groups
    pair = shard // groups
    me = dp_ref[0]
    writer = writer_ref[...]
    named = ones_where(offsets_ref[...] == iota((rows, rows), 0))
    holder = (iota((8, rows), 1) // shard).astype(jnp.float32).astype(jnp.bfloat16)
    source = lax.dot_general(holder, named, NT, preferred_element_type=jnp.float32)
    source = source[:1].astype(jnp.int32)
    kinds = iota((groups * groups, rows), 0)
    member = kinds == writer * groups + source
    earlier = ones_where(iota((rows, rows), 0) < iota((rows, rows), 1))
    before = dot(ones_where(member), earlier)
    count = jnp.sum(jnp.where(member, before, 0.0), axis=0, keepdims=True).astype(jnp.int32)
    within = jnp.sum(
        jnp.where(kinds // groups == writer, before, 0.0), axis=0, keepdims=True
    ).astype(jnp.int32)
    spots = iota((shard, rows), 0)
    mine = offsets_ref[:, pl.ds(pl.multiple_of(me * shard, LANES), shard)]
    leaving = ones_where((writer * pair + count == spots) & (source == me))
    send = dot(leaving, ones_where(mine == iota((rows, shard), 0)))
    send_ref[...] = send.astype(jnp.bfloat16)
    slots = ones_where((within == spots) & (writer == me))
    arrivals = ones_where(source * pair + count == spots)
    place = lax.dot_general(slots, arrivals, NT, preferred_element_type=jnp.float32)
    place_ref[...] = place.astype(jnp.bfloat16)


def copy(src, dst, sem):
    return pltpu.make_async_copy(src, dst, sem)


def split_kernel(count, start, ep_ref, w_ref, m_ref, v_ref, *rest):
    outs, (held, rounded, in_sem, out_sem) = rest[:count], rest[count:]
    height, width = outs[0].shape[1:]
    me = ep_ref[0]
    order = list(range(1, count)) + [0]
    for k in order:
        at = pl.multiple_of((me ^ k) * height, height)
        for f, ref in enumerate((w_ref, m_ref, v_ref)):
            copy(
                ref.at[0, pl.ds(at, height), pl.ds(start, width)],
                held.at[k, f],
                in_sem.at[k, f],
            ).start()
    for k in order:
        for f in range(FIELDS):
            source = w_ref.at[0, pl.ds(0, height), pl.ds(start, width)]
            copy(source, held.at[k, f], in_sem.at[k, f]).wait()
        rounded[k] = held[k].astype(jnp.bfloat16)
        copy(rounded.at[k], outs[k], out_sem.at[k]).start()
    for k in order:
        copy(rounded.at[k], outs[k], out_sem.at[k]).wait()


def sort_kernel(count, start, groups, dp_ref, send_ref, w_ref, m_ref, v_ref, *rest):
    outs, (held, ordered, in_sem, out_sem) = rest[:count], rest[count:]
    height, width = outs[0].shape[1:]
    parts = count // groups
    me = dp_ref[0]
    ins = [
        copy(ref.at[0, :, pl.ds(start, width)], held.at[f], in_sem.at[f])
        for f, ref in enumerate((w_ref, m_ref, v_ref))
    ]
    for one in ins:
        one.start()
    out = []
    for f in range(FIELDS):
        ins[f].wait()
        ordered[f] = dot(send_ref[...], held[f].astype(jnp.bfloat16)).astype(jnp.bfloat16)
        for k in range(count):
            at = pl.multiple_of(((me * parts) ^ k) * height, height)
            one = copy(ordered.at[f, pl.ds(at, height)], outs[k].at[f], out_sem.at[f, k])
            one.start()
            out.append(one)
    for one in out:
        one.wait()


def pick_kernel(count, pick_ref, *rest):
    ins, outs, sem = rest[:count], rest[count : 2 * count], rest[2 * count]
    for k in range(count):
        chosen = pick_ref[k]
        for j in range(count):

            @pl.when(chosen == j)
            def _():
                copy(ins[j], outs[k], sem.at[k]).start()

    for k in range(count):
        copy(ins[0], outs[k], sem.at[k]).wait()


def gather_rows(at_ref, ins, held, sem):
    height = ins[0].shape[1]
    copies = []
    for f in range(FIELDS):
        for k, ref in enumerate(ins):
            at = pl.multiple_of(at_ref[k] * height, height)
            one = copy(ref.at[f], held.at[f, pl.ds(at, height)], sem.at[f, k])
            one.start()
            copies.append(one)
    return copies


def route_kernel(count, groups, at_ref, dp_ref, send_ref, *rest):
    ins, outs = rest[:count], rest[count : count + groups]
    held, ordered, in_sem, out_sem = rest[count + groups :]
    height = outs[0].shape[1]
    me = dp_ref[0]
    copies = gather_rows(at_ref, ins, held, in_sem)
    out = []
    for f in range(FIELDS):
        for one in copies[f * count : (f + 1) * count]:
            one.wait()
        ordered[f] = dot(send_ref[...], held[f]).astype(jnp.bfloat16)
        for k in range(groups):
            at = pl.multiple_of((me ^ k) * height, height)
            one = copy(ordered.at[f, pl.ds(at, height)], outs[k].at[f], out_sem.at[f, k])
            one.start()
            out.append(one)
    for one in out:
        one.wait()


def final_kernel(count, start, fresh, at_ref, place_ref, *rest):
    ins = rest[:count]
    saved, held, ordered, in_sem, out_sem = rest[count if fresh else count + 1 :]
    width = ins[0].shape[2]
    copies = gather_rows(at_ref, ins, held, in_sem)
    out = []
    for f in range(FIELDS):
        for one in copies[f * count : (f + 1) * count]:
            one.wait()
        ordered[f] = dot(place_ref[...], held[f]).astype(jnp.bfloat16)
        one = copy(ordered.at[f], saved.at[f, 0, :, pl.ds(start, width)], out_sem.at[f])
        one.start()
        out.append(one)
    for one in out:
        one.wait()


def swap(piece, axis, size, shift):
    return lax.ppermute(piece, axis, [(i, i ^ shift) for i in range(size)])


def spread(pieces, ep):
    return [pieces[0]] + [swap(pieces[k], "ep", ep, k) for k in range(1, ep)]


def bf16(*shape):
    return jax.ShapeDtypeStruct(shape, jnp.bfloat16)


def on_device(ep, dp, chunks, w, m, v, expert_ids, bucket_offsets, writer_rank):
    _, shard, cols = w.shape
    rows = bucket_offsets.shape[0]
    part = shard // ep
    block = shard // dp
    halves = ep // dp
    e = lax.axis_index("ep").astype(jnp.int32)
    d = lax.axis_index("dp").astype(jnp.int32)
    e1, d1 = e[None], d[None]

    numbers = jnp.arange(ep, dtype=jnp.int32)
    rank = jnp.sum((expert_ids[None, :] < expert_ids[:, None]).astype(jnp.int32), axis=1)
    target = numbers ^ e
    pick = jnp.sum(jnp.where(rank[None, :] == target[:, None], numbers[None, :], 0), axis=1) ^ e
    part_at = target
    block_at = jnp.arange(dp, dtype=jnp.int32) ^ d
    piece_at = pick[0] ^ numbers ^ (halves * d)

    send, place = pl.pallas_call(
        functools.partial(plan_kernel, dp),
        out_shape=(bf16(shard, shard), bf16(shard, shard)),
        in_specs=[SMEM, VMEM, VMEM],
        out_specs=(VMEM, VMEM),
        name="plan",
    )(d1, bucket_offsets.reshape(1, rows), writer_rank.reshape(1, rows))

    def sems(*shape):
        return pltpu.SemaphoreType.DMA(shape)

    def room(width, dtype=jnp.bfloat16):
        return pltpu.VMEM((FIELDS, shard, width), dtype)

    def split(start, width):
        return pl.pallas_call(
            functools.partial(split_kernel, ep, start),
            out_shape=(bf16(FIELDS, part, width),) * ep,
            in_specs=[SMEM, ANY, ANY, ANY],
            out_specs=(ANY,) * ep,
            scratch_shapes=[
                pltpu.VMEM((ep, FIELDS, part, width), jnp.float32),
                pltpu.VMEM((ep, FIELDS, part, width), jnp.bfloat16),
                sems(ep, FIELDS),
                sems(ep),
            ],
            name="split",
        )(e1, w, m, v)

    def sort(start, width):
        return pl.pallas_call(
            functools.partial(sort_kernel, ep, start, dp),
            out_shape=(bf16(FIELDS, part, width),) * ep,
            in_specs=[SMEM, VMEM, ANY, ANY, ANY],
            out_specs=(ANY,) * ep,
            scratch_shapes=[room(width, jnp.float32), room(width), sems(FIELDS), sems(FIELDS, ep)],
            name="sort",
        )(d1, send, w, m, v)

    def choose(pieces):
        return pl.pallas_call(
            functools.partial(pick_kernel, ep),
            out_shape=(bf16(*pieces[0].shape),) * ep,
            in_specs=[SMEM] + [ANY] * ep,
            out_specs=(ANY,) * ep,
            scratch_shapes=[sems(ep)],
            name="choose",
        )(pick, *pieces)

    def route(pieces):
        width = pieces[0].shape[2]
        return pl.pallas_call(
            functools.partial(route_kernel, ep, dp),
            out_shape=(bf16(FIELDS, block, width),) * dp,
            in_specs=[SMEM, SMEM, VMEM] + [ANY] * ep,
            out_specs=(ANY,) * dp,
            scratch_shapes=[room(width), room(width), sems(FIELDS, ep), sems(FIELDS, dp)],
            name="route",
        )(part_at, d1, send, *pieces)

    def finish(saved, at, pieces, start):
        width = pieces[0].shape[2]
        count = len(pieces)
        fresh = saved is None
        return pl.pallas_call(
            functools.partial(final_kernel, count, start, fresh),
            out_shape=bf16(FIELDS, 1, shard, cols),
            in_specs=[SMEM, VMEM] + [ANY] * (count if fresh else count + 1),
            out_specs=ANY,
            scratch_shapes=[room(width), room(width), sems(FIELDS, count), sems(FIELDS)],
            input_output_aliases={} if fresh else {2 + count: 0},
            name="finish",
        )(at, place, *pieces, *(() if fresh else (saved,)))

    def across(pieces, step):
        return [
            piece if k < step else swap(piece, "dp", dp, k // step)
            for k, piece in enumerate(pieces)
        ]

    done = []
    at = 0
    for kind, width in chunks:
        if kind == "ep":
            pieces = spread(split(at, width), ep)
            pieces = spread(choose(pieces), ep)
            pieces = across(route(pieces), 1)
            done.append((block_at, pieces, at))
        else:
            pieces = across(sort(at, width), halves)
            pieces = spread(pieces, ep)
            pieces = spread(choose(pieces), ep)
            done.append((piece_at, pieces, at))
        at += width
    saved = None
    for where, pieces, start in done:
        saved = finish(saved, where, pieces, start)
    return saved


def plain_destinations(bucket_offsets, writer_rank, shard_rows, groups):
    indicator = (writer_rank[:, None] == jnp.arange(groups, dtype=jnp.int32)[None, :]).astype(jnp.int32)
    before = jnp.cumsum(indicator, axis=0) - indicator
    within = jnp.sum(before * indicator, axis=1)
    return jnp.take(writer_rank * shard_rows + within, bucket_offsets)


def plain_route(stacked, target, shard_rows, groups):
    mine = lax.axis_index("dp")
    per_pair = shard_rows // groups
    table = target.reshape(groups, shard_rows)
    outgoing = jnp.argsort(lax.dynamic_index_in_dim(table, mine, 0, keepdims=False))
    sending = jnp.take(stacked, outgoing, axis=1).reshape(FIELDS, groups, per_pair, stacked.shape[2])
    arrived = lax.all_to_all(sending, "dp", split_axis=1, concat_axis=1, tiled=True)
    ordered = jnp.sort(table, axis=1)
    slots = lax.dynamic_slice_in_dim(ordered, mine * per_pair, per_pair, 1).reshape(shard_rows)
    slots = slots - mine * shard_rows
    return jnp.take(arrived.reshape(FIELDS, shard_rows, stacked.shape[2]), jnp.argsort(slots), axis=1)


def plain_on_device(w, m, v, expert_ids, bucket_offsets, writer_rank):
    groups = lax.axis_size("dp")
    shard_rows = w.shape[1]
    stacked = jnp.stack([one[0].astype(jnp.bfloat16) for one in (w, m, v)])
    target = plain_destinations(bucket_offsets, writer_rank, shard_rows, groups)
    stacked = plain_route(stacked, target, shard_rows, groups)
    pieces = lax.all_to_all(stacked[None], "ep", split_axis=2, concat_axis=0, tiled=True)
    chosen = jnp.take(pieces, jnp.argsort(expert_ids), axis=0)
    return lax.all_to_all(chosen, "ep", split_axis=0, concat_axis=2, tiled=True)[0][:, None]


def whole_function(mesh, w, m, v, expert_ids, bucket_offsets, writer_rank):
    ep, dp = mesh.shape["ep"], mesh.shape["dp"]
    rows, cols = w.shape[1:]
    shard = rows // dp
    tiles = cols // LANES
    fits = (
        ep & (ep - 1) == 0
        and dp & (dp - 1) == 0
        and ep % dp == 0
        and shard % LANES == 0
        and shard % (16 * ep) == 0
        and cols % LANES == 0
        and tiles >= 2
    )
    if fits:
        kinds = ("ep", "dp")
        widths = [
            LANES * (tiles * (i + 1) // len(kinds) - tiles * i // len(kinds))
            for i in range(len(kinds))
        ]
        body = functools.partial(on_device, ep, dp, tuple(zip(kinds, widths)))
    else:
        body = plain_on_device
    return jax.shard_map(
        body,
        mesh=mesh,
        in_specs=(P("ep", "dp", None), P("ep", "dp", None), P("ep", "dp", None), P(), P(), P()),
        out_specs=P(None, "ep", "dp", None),
        check_vma=False,
    )(w, m, v, expert_ids, bucket_offsets, writer_rank)


def solution(mesh):
    return functools.partial(whole_function, mesh)
```

```python
import functools

import jax
import jax.numpy as jnp
from jax import lax
from jax.experimental import pallas as pl
from jax.experimental.pallas import tpu as pltpu
from jax.sharding import PartitionSpec as P


FIELDS = 3
LANES = 128
ROOM = 24 * 2**20
HBM = pl.BlockSpec(memory_space=pltpu.HBM)
SMEM = pl.BlockSpec(memory_space=pltpu.SMEM)
VMEM = pl.BlockSpec(memory_space=pltpu.VMEM)
NT = (((1,), (1,)), ((), ()))


def iota(shape, dim):
    return lax.broadcasted_iota(jnp.int32, shape, dim)


def ones_where(mask):
    return jnp.where(mask, 1.0, 0.0).astype(jnp.bfloat16)


def dot(a, b):
    return jnp.dot(a, b, preferred_element_type=jnp.float32)


def plan_kernel(groups, dp_ref, offsets_ref, writer_ref, *rest):
    send_ref, place_ref = rest[-2:]
    rows = offsets_ref.shape[1]
    shard = rows // groups
    pair = shard // groups
    me = dp_ref[0]
    writer = writer_ref[...]
    named = ones_where(offsets_ref[...] == iota((rows, rows), 0))
    holder = (iota((8, rows), 1) // shard).astype(jnp.float32).astype(jnp.bfloat16)
    source = lax.dot_general(holder, named, NT, preferred_element_type=jnp.float32)
    source = source[:1].astype(jnp.int32)
    kinds = iota((groups * groups, rows), 0)
    member = kinds == writer * groups + source
    earlier = ones_where(iota((rows, rows), 0) < iota((rows, rows), 1))
    before = dot(ones_where(member), earlier)
    count = jnp.sum(jnp.where(member, before, 0.0), axis=0, keepdims=True).astype(jnp.int32)
    within = jnp.sum(
        jnp.where(kinds // groups == writer, before, 0.0), axis=0, keepdims=True
    ).astype(jnp.int32)
    spots = iota((shard, rows), 0)
    mine = offsets_ref[:, pl.ds(pl.multiple_of(me * shard, LANES), shard)]
    leaving = ones_where((writer * pair + count == spots) & (source == me))
    send = dot(leaving, ones_where(mine == iota((rows, shard), 0)))
    send_ref[...] = send.astype(jnp.bfloat16)
    slots = ones_where((within == spots) & (writer == me))
    arrivals = ones_where(source * pair + count == spots)
    place = lax.dot_general(slots, arrivals, NT, preferred_element_type=jnp.float32)
    place_ref[...] = place.astype(jnp.bfloat16)


def copy(src, dst, sem):
    return pltpu.make_async_copy(src, dst, sem)


def split_kernel(count, start, ep_ref, w_ref, m_ref, v_ref, *rest):
    outs, (held, sem) = rest[-count - 2 : -2], rest[-2:]
    height, width = outs[0].shape[1:]
    me = ep_ref[0]
    copies = {}
    order = list(range(1, count)) + [0]
    for k in order:
        at = pl.multiple_of((me ^ k) * height, height)
        for f, ref in enumerate((w_ref, m_ref, v_ref)):
            source = ref.at[0, pl.ds(at, height), pl.ds(start, width)]
            copies[k, f] = copy(source, held.at[k, f], sem.at[k, f])
            copies[k, f].start()
    for k in order:
        for f in range(FIELDS):
            copies[k, f].wait()
            outs[k][f] = held[k, f].astype(jnp.bfloat16)


def deal(me, pieces, ordered, outs):
    height = outs[0].shape[1]
    for k in range(pieces):
        at = pl.multiple_of((me ^ k) * height, height)
        for f in range(FIELDS):
            outs[k][f] = ordered[f, pl.ds(at, height)]


def join(at_ref, ins, held):
    height = ins[0].shape[1]
    for k, ref in enumerate(ins):
        at = pl.multiple_of(at_ref[k] * height, height)
        for f in range(FIELDS):
            held[f, pl.ds(at, height)] = ref[f]


def sort_kernel(count, start, groups, dp_ref, send_ref, w_ref, m_ref, v_ref, *rest):
    outs, (held, ordered, sem) = rest[-count - 3 : -3], rest[-3:]
    width = outs[0].shape[2]
    ins = [
        copy(ref.at[0, :, pl.ds(start, width)], held.at[f], sem.at[f])
        for f, ref in enumerate((w_ref, m_ref, v_ref))
    ]
    for one in ins:
        one.start()
    for f in range(FIELDS):
        ins[f].wait()
        ordered[f] = dot(send_ref[...], held[f].astype(jnp.bfloat16)).astype(jnp.bfloat16)
    deal(dp_ref[0] * (count // groups), count, ordered, outs)


def pick_kernel(count, pick_ref, *rest):
    ins, outs = rest[:count], rest[-count:]
    for k in range(count):
        chosen = pick_ref[k]
        for j in range(count):

            @pl.when(chosen == j)
            def _():
                outs[k][...] = ins[j][...]


def route_kernel(count, groups, at_ref, dp_ref, send_ref, *rest):
    ins, outs = rest[:count], rest[-groups - 2 : -2]
    held, ordered = rest[-2:]
    join(at_ref, ins, held)
    for f in range(FIELDS):
        ordered[f] = dot(send_ref[...], held[f]).astype(jnp.bfloat16)
    deal(dp_ref[0], groups, ordered, outs)


def final_kernel(count, start, at_ref, place_ref, *rest):
    ins = rest[:count]
    saved, held, ordered, sem = rest[-4:]
    width = ins[0].shape[2]
    join(at_ref, ins, held)
    out = []
    for f in range(FIELDS):
        ordered[f] = dot(place_ref[...], held[f]).astype(jnp.bfloat16)
        one = copy(ordered.at[f], saved.at[f, 0, :, pl.ds(start, width)], sem.at[f])
        one.start()
        out.append(one)
    for one in out:
        one.wait()


def swap(piece, axis, size, shift):
    return lax.ppermute(piece, axis, [(i, i ^ shift) for i in range(size)])


def spread(pieces, ep):
    return [pieces[0]] + [swap(pieces[k], "ep", ep, k) for k in range(1, ep)]


def bf16(*shape):
    return jax.ShapeDtypeStruct(shape, jnp.bfloat16)


def on_device(ep, dp, chunks, *args):
    return exchange(ep, dp, chunks, *args)


def exchange(ep, dp, chunks, w, m, v, expert_ids, bucket_offsets, writer_rank):
    _, shard, cols = w.shape
    rows = bucket_offsets.shape[0]
    part = shard // ep
    block = shard // dp
    halves = ep // dp
    e = lax.axis_index("ep").astype(jnp.int32)
    d = lax.axis_index("dp").astype(jnp.int32)
    e1, d1 = e[None], d[None]

    numbers = jnp.arange(ep, dtype=jnp.int32)
    rank = jnp.sum((expert_ids[None, :] < expert_ids[:, None]).astype(jnp.int32), axis=1)
    target = numbers ^ e
    pick = jnp.sum(jnp.where(rank[None, :] == target[:, None], numbers[None, :], 0), axis=1) ^ e
    part_at = target
    block_at = jnp.arange(dp, dtype=jnp.int32) ^ d
    piece_at = pick[0] ^ numbers ^ (halves * d)

    def sems(*shape):
        return pltpu.SemaphoreType.DMA(shape)

    def room(width, dtype=jnp.bfloat16):
        return pltpu.VMEM((FIELDS, shard, width), dtype)

    last = []

    def call(kernel, outs, scratch, specs, args, out_space=pltpu.VMEM, **options):
        specs = specs + [pl.BlockSpec(memory_space=out_space)] * len(last)
        args = [
            one if spec is SMEM else pltpu.with_memory_space_constraint(one, spec.memory_space)
            for spec, one in zip(specs, (*args, *last))
        ]
        results = pl.pallas_call(
            kernel,
            out_shape=jax.tree.map(lambda one: out_space(one.shape, one.dtype), outs),
            in_specs=specs,
            out_specs=jax.tree.map(lambda _: pl.BlockSpec(memory_space=out_space), outs),
            scratch_shapes=scratch,
            compiler_params=pltpu.CompilerParams(vmem_limit_bytes=ROOM),
            **options,
        )(*args)
        last[:] = jax.tree.leaves(results)[-1:]
        return results

    def plan():
        return call(
            functools.partial(plan_kernel, dp),
            (bf16(shard, shard), bf16(shard, shard)),
            [],
            [SMEM, VMEM, VMEM],
            (d1, bucket_offsets.reshape(1, rows), writer_rank.reshape(1, rows)),
        )

    def split(start, width):
        return call(
            functools.partial(split_kernel, ep, start),
            (bf16(FIELDS, part, width),) * ep,
            [pltpu.VMEM((ep, FIELDS, part, width), jnp.float32), sems(ep, FIELDS)],
            [SMEM, HBM, HBM, HBM],
            (e1, w, m, v),
        )

    def sort(start, width):
        return call(
            functools.partial(sort_kernel, ep, start, dp),
            (bf16(FIELDS, part, width),) * ep,
            [room(width, jnp.float32), room(width), sems(FIELDS)],
            [SMEM, VMEM, HBM, HBM, HBM],
            (d1, send, w, m, v),
        )

    def choose(pieces):
        return call(
            functools.partial(pick_kernel, ep),
            (bf16(*pieces[0].shape),) * ep,
            [],
            [SMEM] + [VMEM] * ep,
            (pick, *pieces),
        )

    def route(pieces):
        width = pieces[0].shape[2]
        return call(
            functools.partial(route_kernel, ep, dp),
            (bf16(FIELDS, block, width),) * dp,
            [room(width), room(width)],
            [SMEM, SMEM, VMEM] + [VMEM] * ep,
            (part_at, d1, send, *pieces),
        )

    def finish(at, pieces, start):
        width = pieces[0].shape[2]
        count = len(pieces)
        last[:] = saved
        saved[:] = [
            call(
                functools.partial(final_kernel, count, start),
                bf16(FIELDS, 1, shard, cols),
                [room(width), room(width), sems(FIELDS)],
                [SMEM, VMEM] + [VMEM] * count,
                (at, place, *pieces),
                pltpu.HBM,
                **({"input_output_aliases": {2 + count: 0}} if saved else {}),
            )
        ]

    def across(pieces, step):
        far = {}
        for shift in list(range(2, dp)) + [1]:
            for k in range(shift * step, shift * step + step):
                far[k] = swap(pieces[k], "dp", dp, shift)
        return [far.get(k, piece) for k, piece in enumerate(pieces)]

    saved = []
    (c, cw), (g, gw) = [(a, n) for k, a, n in chunks if k == "ep"]
    (a, aw), (b, bw) = [(a, n) for k, a, n in chunks if k == "dp"]

    c_parts = split(c, cw)
    c_parts = spread(c_parts, ep)
    send, place = plan()
    a_parts = sort(a, aw)
    a_parts = across(a_parts, halves)
    g_parts = split(g, gw)
    g_parts = spread(g_parts, ep)
    c_parts = choose(c_parts)
    c_parts = spread(c_parts, ep)
    b_parts = sort(b, bw)
    b_parts = across(b_parts, halves)
    g_parts = choose(g_parts)
    g_parts = spread(g_parts, ep)
    c_parts = route(c_parts)
    c_parts = across(c_parts, 1)
    a_parts = spread(a_parts, ep)
    g_parts = route(g_parts)
    g_parts = across(g_parts, 1)
    b_parts = spread(b_parts, ep)
    a_parts = choose(a_parts)
    a_parts = spread(a_parts, ep)
    b_parts = choose(b_parts)
    b_parts = spread(b_parts, ep)
    finish(block_at, c_parts, c)
    finish(piece_at, a_parts, a)
    finish(piece_at, b_parts, b)
    finish(block_at, g_parts, g)
    return saved[0]


def plain_destinations(bucket_offsets, writer_rank, shard_rows, groups):
    indicator = (writer_rank[:, None] == jnp.arange(groups, dtype=jnp.int32)[None, :]).astype(jnp.int32)
    before = jnp.cumsum(indicator, axis=0) - indicator
    within = jnp.sum(before * indicator, axis=1)
    return jnp.take(writer_rank * shard_rows + within, bucket_offsets)


def plain_route(stacked, target, shard_rows, groups):
    mine = lax.axis_index("dp")
    per_pair = shard_rows // groups
    table = target.reshape(groups, shard_rows)
    outgoing = jnp.argsort(lax.dynamic_index_in_dim(table, mine, 0, keepdims=False))
    sending = jnp.take(stacked, outgoing, axis=1).reshape(FIELDS, groups, per_pair, stacked.shape[2])
    arrived = lax.all_to_all(sending, "dp", split_axis=1, concat_axis=1, tiled=True)
    ordered = jnp.sort(table, axis=1)
    slots = lax.dynamic_slice_in_dim(ordered, mine * per_pair, per_pair, 1).reshape(shard_rows)
    slots = slots - mine * shard_rows
    return jnp.take(arrived.reshape(FIELDS, shard_rows, stacked.shape[2]), jnp.argsort(slots), axis=1)


def plain_on_device(w, m, v, expert_ids, bucket_offsets, writer_rank):
    groups = lax.axis_size("dp")
    shard_rows = w.shape[1]
    stacked = jnp.stack([one[0].astype(jnp.bfloat16) for one in (w, m, v)])
    target = plain_destinations(bucket_offsets, writer_rank, shard_rows, groups)
    stacked = plain_route(stacked, target, shard_rows, groups)
    pieces = lax.all_to_all(stacked[None], "ep", split_axis=2, concat_axis=0, tiled=True)
    chosen = jnp.take(pieces, jnp.argsort(expert_ids), axis=0)
    return lax.all_to_all(chosen, "ep", split_axis=0, concat_axis=2, tiled=True)[0][:, None]


def solution(mesh):
    ep, dp = mesh.shape["ep"], mesh.shape["dp"]
    specs = dict(
        mesh=mesh,
        in_specs=(P("ep", "dp", None), P("ep", "dp", None), P("ep", "dp", None), P(), P(), P()),
        out_specs=P(None, "ep", "dp", None),
        check_vma=False,
    )

    def fits(rows, cols):
        shard = rows // dp
        return (
            ep & (ep - 1) == 0
            and dp & (dp - 1) == 0
            and ep % dp == 0
            and shard % LANES == 0
            and shard % (16 * ep) == 0
            and cols % (4 * LANES) == 0
        )

    def function(w, m, v, expert_ids, bucket_offsets, writer_rank):
        rows, cols = w.shape[1:]
        args = (w, m, v, expert_ids, bucket_offsets, writer_rank)
        if not fits(rows, cols):
            return jax.shard_map(plain_on_device, **specs)(*args)
        kinds = ("ep", "ep", "dp", "dp")
        tiles = cols // LANES
        edges = [LANES * (tiles * i // len(kinds)) for i in range(len(kinds) + 1)]
        chunks = tuple((kind, edges[i], edges[i + 1] - edges[i]) for i, kind in enumerate(kinds))
        body = jax.shard_map(functools.partial(on_device, ep, dp, chunks), **specs)
        return body(*args)

    return function
```

```python
import functools

import jax
import jax.numpy as jnp
from jax import lax
from jax.experimental import pallas as pl
from jax.experimental.pallas import tpu as pltpu
from jax.sharding import PartitionSpec as P


FIELDS = 3
LANES = 128
ROOM = 24 * 2**20
SHARES = (9, 5, 9, 5)
HBM = pl.BlockSpec(memory_space=pltpu.HBM)
SMEM = pl.BlockSpec(memory_space=pltpu.SMEM)
VMEM = pl.BlockSpec(memory_space=pltpu.VMEM)
NT = (((1,), (1,)), ((), ()))


def iota(shape, dim):
    return lax.broadcasted_iota(jnp.int32, shape, dim)


def ones_where(mask):
    return jnp.where(mask, 1.0, 0.0).astype(jnp.bfloat16)


def dot(a, b):
    return jnp.dot(a, b, preferred_element_type=jnp.float32)


def plan(groups, dp_ref, offsets_ref, writer_ref, send_ref, place_ref):
    rows = offsets_ref.shape[1]
    shard = rows // groups
    pair = shard // groups
    me = dp_ref[0]
    writer = writer_ref[...]
    offsets = offsets_ref[...]
    high = jnp.where(offsets // LANES == iota((rows // LANES, rows), 0), iota((1, rows), 1) // shard, 0)
    low = ones_where(offsets % LANES == iota((LANES, rows), 0))
    high = high.astype(jnp.float32).astype(jnp.bfloat16)
    source = lax.dot_general(high, low, NT, preferred_element_type=jnp.float32).astype(jnp.int32)
    source = jnp.concatenate([source[i : i + 1] for i in range(rows // LANES)], axis=1)
    kinds = iota((groups * groups, rows), 0)
    member = jnp.where(kinds == writer * groups + source, 1.0, 0.0)
    earlier = ones_where(iota((LANES, LANES), 0) < iota((LANES, LANES), 1))
    before, total = [], jnp.zeros((groups * groups, 1), jnp.float32)
    for i in range(rows // LANES):
        some = member[:, i * LANES : (i + 1) * LANES]
        before.append(dot(some.astype(jnp.bfloat16), earlier) + total)
        total = total + jnp.sum(some, axis=1, keepdims=True)
    before = jnp.concatenate(before, axis=1)
    count = jnp.sum(member * before, axis=0, keepdims=True).astype(jnp.int32)
    within = jnp.sum(
        jnp.where(kinds // groups == writer, before, 0.0), axis=0, keepdims=True
    ).astype(jnp.int32)
    spots = iota((shard, rows), 0)
    mine = offsets_ref[:, pl.ds(pl.multiple_of(me * shard, LANES), shard)]
    leaving = ones_where(((writer ^ me) * pair + count == spots) & (source == me))
    send = dot(leaving, ones_where(mine == iota((rows, shard), 0)))
    send_ref[...] = send.astype(jnp.bfloat16)
    slots = ones_where((within == spots) & (writer == me))
    arrivals = ones_where((source ^ me) * pair + count == spots)
    place = lax.dot_general(slots, arrivals, NT, preferred_element_type=jnp.float32)
    place_ref[...] = place.astype(jnp.bfloat16)


def copy(src, dst, sem):
    return pltpu.make_async_copy(src, dst, sem)


def part_copies(start, ep_ref, refs, held, sem):
    count, _, height, width = held.shape
    me = ep_ref[0]
    copies = []
    for k in range(count):
        at = pl.multiple_of((me ^ k) * height, height)
        for f, ref in enumerate(refs):
            source = ref.at[0, pl.ds(at, height), pl.ds(start, width)]
            copies.append(copy(source, held.at[k, f], sem.at[k, f]))
    for one in copies:
        one.start()
    return copies


def round_parts(copies, held, outs):
    for k, out in enumerate(outs):
        for f in range(FIELDS):
            copies[k * FIELDS + f].wait()
            out[f] = held[k, f].astype(jnp.bfloat16)


def row_copies(start, refs, held, sem):
    width = held.shape[2]
    copies = [
        copy(ref.at[0, :, pl.ds(start, width)], held.at[f], sem.at[f]) for f, ref in enumerate(refs)
    ]
    for one in copies:
        one.start()
    return copies


def sort_rows(copies, send_ref, held, outs):
    for f in range(FIELDS):
        copies[f].wait()
        deal(dot(send_ref[...], held[f].astype(jnp.bfloat16)), f, outs)


def first_kernel(
    count, groups, parts_start, rows_start, ep_ref, dp_ref, offsets_ref, writer_ref, w_ref, m_ref, v_ref, *rest
):
    parts_out, rows_out = rest[:count], rest[count : 2 * count]
    send_ref, place_ref, offsets, writer, parts_held, rows_held, table_sem, parts_sem, rows_sem = rest[2 * count :]
    refs = (w_ref, m_ref, v_ref)
    tables = [copy(offsets_ref, offsets, table_sem.at[0]), copy(writer_ref, writer, table_sem.at[1])]
    for one in tables:
        one.start()
    parts = part_copies(parts_start, ep_ref, refs, parts_held, parts_sem)
    rows = row_copies(rows_start, refs, rows_held, rows_sem)
    for one in tables:
        one.wait()
    plan(groups, dp_ref, offsets, writer, send_ref, place_ref)
    round_parts(parts, parts_held, parts_out)
    sort_rows(rows, send_ref, rows_held, rows_out)


def split_kernel(count, start, ep_ref, w_ref, m_ref, v_ref, *rest):
    outs, (held, sem) = rest[-count - 2 : -2], rest[-2:]
    copies = part_copies(start, ep_ref, (w_ref, m_ref, v_ref), held, sem)
    round_parts(copies, held, outs)


def deal(rows, f, outs):
    height = outs[0].shape[1]
    for k, out in enumerate(outs):
        out[f] = rows[k * height : (k + 1) * height].astype(jnp.bfloat16)


def join(at_ref, ins, held):
    height = ins[0].shape[1]
    for k, ref in enumerate(ins):
        at = pl.multiple_of(at_ref[k] * height, height)
        for f in range(FIELDS):
            held[f, pl.ds(at, height)] = ref[f]


def sort_kernel(count, start, send_ref, w_ref, m_ref, v_ref, *rest):
    outs, (held, sem) = rest[-count - 2 : -2], rest[-2:]
    sort_rows(row_copies(start, (w_ref, m_ref, v_ref), held, sem), send_ref, held, outs)


def pick_kernel(count, pick_ref, *rest):
    ins, outs = rest[:count], rest[-count:]
    for k in range(count):
        chosen = pick_ref[k]
        for j in range(count):

            @pl.when(chosen == j)
            def _():
                outs[k][...] = ins[j][...]


def route_kernel(count, groups, at_ref, send_ref, *rest):
    ins, outs, held = rest[:count], rest[-groups - 1 : -1], rest[-1]
    join(at_ref, ins, held)
    for f in range(FIELDS):
        deal(dot(send_ref[...], held[f]), f, outs)


def final_kernel(counts, starts, place_ref, *rest):
    chunks = len(counts)
    ats, rest = rest[:chunks], rest[chunks:]
    saved, scratch, sem = rest[-2 * chunks - 2], rest[-2 * chunks - 1 : -1], rest[-1]
    out = []
    for i, count in enumerate(counts):
        ins, rest = rest[:count], rest[count:]
        held, ordered = scratch[2 * i], scratch[2 * i + 1]
        width = held.shape[2]
        join(ats[i], ins, held)
        for f in range(FIELDS):
            ordered[f] = dot(place_ref[...], held[f]).astype(jnp.bfloat16)
            one = copy(ordered.at[f], saved.at[f, 0, :, pl.ds(starts[i], width)], sem.at[i, f])
            one.start()
            out.append(one)
    for one in out:
        one.wait()


def swap(piece, axis, size, shift):
    return lax.ppermute(piece, axis, [(i, i ^ shift) for i in range(size)])


def far_first(size):
    return list(range(2, size)) + [1]


def wide_order(ep):
    return sorted(range(2, ep), key=lambda k: ((k // 2).bit_count() > 1, k % 2, k)) + [1]


def spread(pieces, ep):
    far = {k: swap(pieces[k], "ep", ep, k) for k in wide_order(ep)}
    return [far.get(k, piece) for k, piece in enumerate(pieces)]


def bf16(*shape):
    return jax.ShapeDtypeStruct(shape, jnp.bfloat16)


def on_device(ep, dp, chunks, *args):
    return exchange(ep, dp, chunks, *args)


def exchange(ep, dp, chunks, w, m, v, expert_ids, bucket_offsets, writer_rank):
    _, shard, cols = w.shape
    rows = bucket_offsets.shape[0]
    part = shard // ep
    block = shard // dp
    halves = ep // dp
    e = lax.axis_index("ep").astype(jnp.int32)
    d = lax.axis_index("dp").astype(jnp.int32)
    e1, d1 = e[None], d[None]

    numbers = jnp.arange(ep, dtype=jnp.int32)
    rank = jnp.sum((expert_ids[None, :] < expert_ids[:, None]).astype(jnp.int32), axis=1)
    target = numbers ^ e
    pick = jnp.sum(jnp.where(rank[None, :] == target[:, None], numbers[None, :], 0), axis=1) ^ e
    part_at = target
    block_at = jnp.arange(dp, dtype=jnp.int32)
    piece_at = pick[0] ^ numbers

    def sems(*shape):
        return pltpu.SemaphoreType.DMA(shape)

    def room(width, dtype=jnp.bfloat16):
        return pltpu.VMEM((FIELDS, shard, width), dtype)

    last = []

    def call(kernel, outs, scratch, specs, args, out_space=pltpu.VMEM, **options):
        specs = specs + [pl.BlockSpec(memory_space=out_space)] * len(last)
        args = [
            one if spec is SMEM else pltpu.with_memory_space_constraint(one, spec.memory_space)
            for spec, one in zip(specs, (*args, *last))
        ]
        results = pl.pallas_call(
            kernel,
            out_shape=jax.tree.map(lambda one: out_space(one.shape, one.dtype), outs),
            in_specs=specs,
            out_specs=jax.tree.map(lambda _: pl.BlockSpec(memory_space=out_space), outs),
            scratch_shapes=scratch,
            compiler_params=pltpu.CompilerParams(vmem_limit_bytes=ROOM),
            **options,
        )(*args)
        last[:] = jax.tree.leaves(results)[-1:]
        return results

    def first(c, cw, a, aw):
        pieces = (ep, FIELDS, part, cw)
        results = call(
            functools.partial(first_kernel, ep, dp, c, a),
            (bf16(FIELDS, part, cw),) * ep + (bf16(FIELDS, part, aw),) * ep + (bf16(shard, shard),) * 2,
            [
                pltpu.VMEM((1, rows), jnp.int32),
                pltpu.VMEM((1, rows), jnp.int32),
                pltpu.VMEM(pieces, jnp.float32),
                room(aw, jnp.float32),
                sems(2),
                sems(ep, FIELDS),
                sems(FIELDS),
            ],
            [SMEM, SMEM, HBM, HBM, HBM, HBM, HBM],
            (e1, d1, bucket_offsets.reshape(1, rows), writer_rank.reshape(1, rows), w, m, v),
        )
        return list(results[:ep]), list(results[ep : 2 * ep]), *results[2 * ep :]

    def split(start, width):
        return call(
            functools.partial(split_kernel, ep, start),
            (bf16(FIELDS, part, width),) * ep,
            [pltpu.VMEM((ep, FIELDS, part, width), jnp.float32), sems(ep, FIELDS)],
            [SMEM, HBM, HBM, HBM],
            (e1, w, m, v),
        )

    def sort(start, width):
        return call(
            functools.partial(sort_kernel, ep, start),
            (bf16(FIELDS, part, width),) * ep,
            [room(width, jnp.float32), sems(FIELDS)],
            [VMEM, HBM, HBM, HBM],
            (send, w, m, v),
        )

    def choose(pieces):
        return call(
            functools.partial(pick_kernel, ep),
            (bf16(*pieces[0].shape),) * ep,
            [],
            [SMEM] + [VMEM] * ep,
            (pick, *pieces),
        )

    def route(pieces):
        width = pieces[0].shape[2]
        return call(
            functools.partial(route_kernel, ep, dp),
            (bf16(FIELDS, block, width),) * dp,
            [room(width)],
            [SMEM, VMEM] + [VMEM] * ep,
            (part_at, send, *pieces),
        )

    def finish(*chunks):
        counts = tuple(len(pieces) for _, pieces, _ in chunks)
        widths = [pieces[0].shape[2] for _, pieces, _ in chunks]
        total = sum(counts)
        last[:] = saved
        saved[:] = [
            call(
                functools.partial(final_kernel, counts, tuple(start for _, _, start in chunks)),
                bf16(FIELDS, 1, shard, cols),
                [room(width) for width in widths for _ in range(2)] + [sems(len(chunks), FIELDS)],
                [VMEM] + [SMEM] * len(chunks) + [VMEM] * total,
                (place, *[at for at, _, _ in chunks], *[one for _, pieces, _ in chunks for one in pieces]),
                pltpu.HBM,
                **({"input_output_aliases": {1 + len(chunks) + total: 0}} if saved else {}),
            )
        ]

    def across(pieces, step):
        far = {}
        for shift in far_first(dp):
            for k in range(shift * step, shift * step + step):
                far[k] = swap(pieces[k], "dp", dp, shift)
        return [far.get(k, piece) for k, piece in enumerate(pieces)]

    saved = []
    (c, cw), (g, gw) = [(a, n) for k, a, n in chunks if k == "ep"]
    (a, aw), (b, bw) = [(a, n) for k, a, n in chunks if k == "dp"]

    c_parts, a_parts, send, place = first(c, cw, a, aw)
    c_parts = spread(c_parts, ep)
    a_parts = across(a_parts, halves)
    g_parts = split(g, gw)
    g_parts = spread(g_parts, ep)
    c_parts = choose(c_parts)
    c_parts = spread(c_parts, ep)
    b_parts = sort(b, bw)
    b_parts = across(b_parts, halves)
    g_parts = choose(g_parts)
    g_parts = spread(g_parts, ep)
    c_parts = route(c_parts)
    c_parts = across(c_parts, 1)
    a_parts = spread(a_parts, ep)
    g_parts = route(g_parts)
    g_parts = across(g_parts, 1)
    b_parts = spread(b_parts, ep)
    a_parts = choose(a_parts)
    a_parts = spread(a_parts, ep)
    b_parts = choose(b_parts)
    b_parts = spread(b_parts, ep)
    finish((block_at, c_parts, c))
    finish((piece_at, a_parts, a))
    finish((piece_at, b_parts, b), (block_at, g_parts, g))
    return saved[0]


def plain_destinations(bucket_offsets, writer_rank, shard_rows, groups):
    indicator = (writer_rank[:, None] == jnp.arange(groups, dtype=jnp.int32)[None, :]).astype(jnp.int32)
    before = jnp.cumsum(indicator, axis=0) - indicator
    within = jnp.sum(before * indicator, axis=1)
    return jnp.take(writer_rank * shard_rows + within, bucket_offsets)


def plain_route(stacked, target, shard_rows, groups):
    mine = lax.axis_index("dp")
    per_pair = shard_rows // groups
    table = target.reshape(groups, shard_rows)
    outgoing = jnp.argsort(lax.dynamic_index_in_dim(table, mine, 0, keepdims=False))
    sending = jnp.take(stacked, outgoing, axis=1).reshape(FIELDS, groups, per_pair, stacked.shape[2])
    arrived = lax.all_to_all(sending, "dp", split_axis=1, concat_axis=1, tiled=True)
    ordered = jnp.sort(table, axis=1)
    slots = lax.dynamic_slice_in_dim(ordered, mine * per_pair, per_pair, 1).reshape(shard_rows)
    slots = slots - mine * shard_rows
    return jnp.take(arrived.reshape(FIELDS, shard_rows, stacked.shape[2]), jnp.argsort(slots), axis=1)


def plain_on_device(w, m, v, expert_ids, bucket_offsets, writer_rank):
    groups = lax.axis_size("dp")
    shard_rows = w.shape[1]
    stacked = jnp.stack([one[0].astype(jnp.bfloat16) for one in (w, m, v)])
    target = plain_destinations(bucket_offsets, writer_rank, shard_rows, groups)
    stacked = plain_route(stacked, target, shard_rows, groups)
    pieces = lax.all_to_all(stacked[None], "ep", split_axis=2, concat_axis=0, tiled=True)
    chosen = jnp.take(pieces, jnp.argsort(expert_ids), axis=0)
    return lax.all_to_all(chosen, "ep", split_axis=0, concat_axis=2, tiled=True)[0][:, None]


def solution(mesh):
    ep, dp = mesh.shape["ep"], mesh.shape["dp"]
    specs = dict(
        mesh=mesh,
        in_specs=(P("ep", "dp", None), P("ep", "dp", None), P("ep", "dp", None), P(), P(), P()),
        out_specs=P(None, "ep", "dp", None),
        check_vma=False,
    )

    def fits(rows, cols):
        shard = rows // dp
        return (
            ep & (ep - 1) == 0
            and dp & (dp - 1) == 0
            and ep % dp == 0
            and shard % LANES == 0
            and shard % (16 * ep) == 0
            and cols % LANES == 0
            and rows % LANES == 0
            and cols // LANES >= sum(SHARES)
        )

    def function(w, m, v, expert_ids, bucket_offsets, writer_rank):
        rows, cols = w.shape[1:]
        args = (w, m, v, expert_ids, bucket_offsets, writer_rank)
        if not fits(rows, cols):
            return jax.shard_map(plain_on_device, **specs)(*args)
        kinds = ("ep", "ep", "dp", "dp")
        tiles = cols // LANES
        edges = [LANES * (tiles * sum(SHARES[:i]) // sum(SHARES)) for i in range(len(SHARES) + 1)]
        chunks = tuple((kind, edges[i], edges[i + 1] - edges[i]) for i, kind in enumerate(kinds))
        body = jax.shard_map(functools.partial(on_device, ep, dp, chunks), **specs)
        return body(*args)

    return function
```

```python
import functools

import jax
import jax.numpy as jnp
from jax import lax
from jax.experimental import pallas as pl
from jax.experimental.pallas import tpu as pltpu
from jax.sharding import PartitionSpec as P


FIELDS = 3
LANES = 128
ROOM = 24 * 2**20
EARLY = 2
SHARES = (9, 5, 9, 5)
HBM = pl.BlockSpec(memory_space=pltpu.HBM)
SMEM = pl.BlockSpec(memory_space=pltpu.SMEM)
VMEM = pl.BlockSpec(memory_space=pltpu.VMEM)
NT = (((1,), (1,)), ((), ()))


def iota(shape, dim):
    return lax.broadcasted_iota(jnp.int32, shape, dim)


def ones_where(mask):
    return jnp.where(mask, 1.0, 0.0).astype(jnp.bfloat16)


def dot(a, b):
    return jnp.dot(a, b, preferred_element_type=jnp.float32)


def plan(groups, dp_ref, offsets_ref, writer_ref, send_ref, place_ref):
    rows = offsets_ref.shape[1]
    shard = rows // groups
    pair = shard // groups
    me = dp_ref[0]
    writer = writer_ref[...]
    offsets = offsets_ref[...]
    high = jnp.where(offsets // LANES == iota((rows // LANES, rows), 0), iota((1, rows), 1) // shard, 0)
    low = ones_where(offsets % LANES == iota((LANES, rows), 0))
    high = high.astype(jnp.float32).astype(jnp.bfloat16)
    source = lax.dot_general(high, low, NT, preferred_element_type=jnp.float32).astype(jnp.int32)
    source = jnp.concatenate([source[i : i + 1] for i in range(rows // LANES)], axis=1)
    kinds = iota((groups * groups, rows), 0)
    member = jnp.where(kinds == writer * groups + source, 1.0, 0.0)
    earlier = ones_where(iota((LANES, LANES), 0) < iota((LANES, LANES), 1))
    before, total = [], jnp.zeros((groups * groups, 1), jnp.float32)
    for i in range(rows // LANES):
        some = member[:, i * LANES : (i + 1) * LANES]
        before.append(dot(some.astype(jnp.bfloat16), earlier) + total)
        total = total + jnp.sum(some, axis=1, keepdims=True)
    before = jnp.concatenate(before, axis=1)
    count = jnp.sum(member * before, axis=0, keepdims=True).astype(jnp.int32)
    within = jnp.sum(
        jnp.where(kinds // groups == writer, before, 0.0), axis=0, keepdims=True
    ).astype(jnp.int32)
    spots = iota((shard, rows), 0)
    mine = offsets_ref[:, pl.ds(pl.multiple_of(me * shard, LANES), shard)]
    leaving = ones_where(((writer ^ me) * pair + count == spots) & (source == me))
    send = dot(leaving, ones_where(mine == iota((rows, shard), 0)))
    send_ref[...] = send.astype(jnp.bfloat16)
    slots = ones_where((within == spots) & (writer == me))
    arrivals = ones_where((source ^ me) * pair + count == spots)
    place = lax.dot_general(slots, arrivals, NT, preferred_element_type=jnp.float32)
    place_ref[...] = place.astype(jnp.bfloat16)


def copy(src, dst, sem):
    return pltpu.make_async_copy(src, dst, sem)


def row_copies(start, refs, held, sem):
    width = held.shape[2]
    copies = [
        copy(ref.at[0, :, pl.ds(start, width)], held.at[f], sem.at[f]) for f, ref in enumerate(refs)
    ]
    for one in copies:
        one.start()
    return copies


def deal(rows, f, outs):
    height = outs[0].shape[1]
    for k, out in enumerate(outs):
        out[f] = rows[k * height : (k + 1) * height].astype(jnp.bfloat16)


def join(at_ref, ins, held):
    height = ins[0].shape[1]
    for k, ref in enumerate(ins):
        at = pl.multiple_of(at_ref[k] * height, height)
        for f in range(FIELDS):
            held[f, pl.ds(at, height)] = ref[f]


def round_parts(ep_ref, copies, held, outs):
    for f in range(FIELDS):
        copies[f].wait()
        for k, out in outs.items():
            height = out.shape[1]
            at = pl.multiple_of((ep_ref[0] ^ k) * height, height)
            out[f] = held[f, pl.ds(at, height)].astype(jnp.bfloat16)


def sort_rows(copies, send_ref, held, outs):
    for f in range(FIELDS):
        copies[f].wait()
        deal(dot(send_ref[...], held[f].astype(jnp.bfloat16)), f, outs)


def first_kernel(
    lead, groups, parts_start, rows_start, ep_ref, dp_ref, offsets_ref, writer_ref, w_ref, m_ref, v_ref, *rest
):
    parts_out, rest = rest[: len(lead)], rest[len(lead) :]
    rows_ref, send_ref, place_ref, offsets, writer, held, table_sem, parts_sem, rows_sem = rest
    refs = (w_ref, m_ref, v_ref)
    height, width = held.shape[2:]
    tables = [copy(offsets_ref, offsets, table_sem.at[0]), copy(writer_ref, writer, table_sem.at[1])]
    parts = []
    for i, k in enumerate(lead):
        at = pl.multiple_of((ep_ref[0] ^ k) * height, height)
        for f, ref in enumerate(refs):
            source = ref.at[0, pl.ds(at, height), pl.ds(parts_start, width)]
            parts.append(copy(source, held.at[i, f], parts_sem.at[i, f]))
    for one in tables + parts:
        one.start()
    rows = row_copies(rows_start, refs, rows_ref, rows_sem)
    for one in tables:
        one.wait()
    plan(groups, dp_ref, offsets, writer, send_ref, place_ref)
    for one in parts:
        one.wait()
    for i, out in enumerate(parts_out):
        out[...] = held[i].astype(jnp.bfloat16)
    for one in rows:
        one.wait()


def lead_kernel(low, send_ref, rows_ref, *rest):
    outs = rest[-low[1] :]
    height = outs[0].shape[1]
    some = send_ref[low[0] * height : (low[0] + low[1]) * height]
    for f in range(FIELDS):
        deal(dot(some, rows_ref[f].astype(jnp.bfloat16)), f, outs)


def rest_kernel(parts_left, rows_left, start, ep_ref, send_ref, rows_ref, w_ref, m_ref, v_ref, *rest):
    outs, (held, sem) = rest[-len(parts_left) - len(rows_left) - 2 : -2], rest[-2:]
    copies = row_copies(start, (w_ref, m_ref, v_ref), held, sem)
    rows_out = outs[len(parts_left) :]
    height = rows_out[0].shape[1]
    for f in range(FIELDS):
        rows = rows_ref[f].astype(jnp.bfloat16)
        ordered = dot(send_ref[...], rows)
        for k, out in zip(rows_left, rows_out):
            out[f] = ordered[k * height : (k + 1) * height].astype(jnp.bfloat16)
    round_parts(ep_ref, copies, held, dict(zip(parts_left, outs)))


def split_kernel(count, start, ep_ref, w_ref, m_ref, v_ref, *rest):
    outs, (held, sem) = rest[-count - 2 : -2], rest[-2:]
    copies = row_copies(start, (w_ref, m_ref, v_ref), held, sem)
    round_parts(ep_ref, copies, held, dict(enumerate(outs)))


def sort_kernel(count, start, send_ref, w_ref, m_ref, v_ref, *rest):
    outs, (held, sem) = rest[-count - 2 : -2], rest[-2:]
    sort_rows(row_copies(start, (w_ref, m_ref, v_ref), held, sem), send_ref, held, outs)


def pick_kernel(count, pick_ref, *rest):
    ins, outs = rest[:count], rest[-count:]
    for k in range(count):
        chosen = pick_ref[k]
        for j in range(count):

            @pl.when(chosen == j)
            def _():
                outs[k][...] = ins[j][...]


def route_kernel(count, groups, at_ref, send_ref, *rest):
    ins, outs, held = rest[:count], rest[-groups - 1 : -1], rest[-1]
    join(at_ref, ins, held)
    for f in range(FIELDS):
        deal(dot(send_ref[...], held[f]), f, outs)


def final_kernel(counts, starts, place_ref, *rest):
    chunks = len(counts)
    ats, rest = rest[:chunks], rest[chunks:]
    saved, scratch, sem = rest[-2 * chunks - 2], rest[-2 * chunks - 1 : -1], rest[-1]
    out = []
    for i, count in enumerate(counts):
        ins, rest = rest[:count], rest[count:]
        held, ordered = scratch[2 * i], scratch[2 * i + 1]
        width = held.shape[2]
        join(ats[i], ins, held)
        for f in range(FIELDS):
            ordered[f] = dot(place_ref[...], held[f]).astype(jnp.bfloat16)
            one = copy(ordered.at[f], saved.at[f, 0, :, pl.ds(starts[i], width)], sem.at[i, f])
            one.start()
            out.append(one)
    for one in out:
        one.wait()


def swap(piece, axis, size, shift):
    return lax.ppermute(piece, axis, [(i, i ^ shift) for i in range(size)])


def far_first(size):
    return list(range(2, size)) + [1]


def farthest_first(size):
    return list(range(size - 1, 0, -1))


def wide_order(ep, both_first=False):
    sign = -1 if both_first else 1
    return sorted(range(2, ep), key=lambda k: (sign * (k // 2).bit_count(), k % 2, k)) + [1]


def spread(pieces, ep):
    far = {k: swap(pieces[k], "ep", ep, k) for k in range(1, ep)}
    return [far.get(k, piece) for k, piece in enumerate(pieces)]


def lead_hops(ep):
    return wide_order(ep, True)[:EARLY]


def bf16(*shape):
    return jax.ShapeDtypeStruct(shape, jnp.bfloat16)


def on_device(ep, dp, chunks, *args):
    return exchange(ep, dp, chunks, *args)


def exchange(ep, dp, chunks, w, m, v, expert_ids, bucket_offsets, writer_rank):
    _, shard, cols = w.shape
    rows = bucket_offsets.shape[0]
    part = shard // ep
    block = shard // dp
    halves = ep // dp
    e = lax.axis_index("ep").astype(jnp.int32)
    d = lax.axis_index("dp").astype(jnp.int32)
    e1, d1 = e[None], d[None]

    numbers = jnp.arange(ep, dtype=jnp.int32)
    rank = jnp.sum((expert_ids[None, :] < expert_ids[:, None]).astype(jnp.int32), axis=1)
    target = numbers ^ e
    pick = jnp.sum(jnp.where(rank[None, :] == target[:, None], numbers[None, :], 0), axis=1) ^ e
    part_at = target
    block_at = jnp.arange(dp, dtype=jnp.int32)
    piece_at = pick[0] ^ numbers

    def sems(*shape):
        return pltpu.SemaphoreType.DMA(shape)

    def room(width, dtype=jnp.bfloat16):
        return pltpu.VMEM((FIELDS, shard, width), dtype)

    last = []

    def call(kernel, outs, scratch, specs, args, out_space=pltpu.VMEM, **options):
        specs = specs + [pl.BlockSpec(memory_space=out_space)] * len(last)
        args = [
            one if spec is SMEM else pltpu.with_memory_space_constraint(one, spec.memory_space)
            for spec, one in zip(specs, (*args, *last))
        ]
        results = pl.pallas_call(
            kernel,
            out_shape=jax.tree.map(lambda one: out_space(one.shape, one.dtype), outs),
            in_specs=specs,
            out_specs=jax.tree.map(lambda _: pl.BlockSpec(memory_space=out_space), outs),
            scratch_shapes=scratch,
            compiler_params=pltpu.CompilerParams(vmem_limit_bytes=ROOM),
            **options,
        )(*args)
        last[:] = jax.tree.leaves(results)[-1:]
        return results

    def first(c, cw, a, aw):
        lead = lead_hops(ep)
        *pieces, held, send, place = call(
            functools.partial(first_kernel, lead, dp, c, a),
            (bf16(FIELDS, part, cw),) * len(lead)
            + (jax.ShapeDtypeStruct((FIELDS, shard, aw), jnp.float32),)
            + (bf16(shard, shard),) * 2,
            [
                pltpu.VMEM((1, rows), jnp.int32),
                pltpu.VMEM((1, rows), jnp.int32),
                pltpu.VMEM((len(lead), FIELDS, part, cw), jnp.float32),
                sems(2),
                sems(len(lead), FIELDS),
                sems(FIELDS),
            ],
            [SMEM, SMEM, HBM, HBM, HBM, HBM, HBM],
            (e1, d1, bucket_offsets.reshape(1, rows), writer_rank.reshape(1, rows), w, m, v),
        )
        return dict(zip(lead, pieces)), held, send, place

    def lead(held):
        low = farthest_first(dp)[0] * halves
        pieces = call(
            functools.partial(lead_kernel, (low, halves)),
            (bf16(FIELDS, part, held.shape[2]),) * halves,
            [],
            [VMEM, VMEM],
            (send, held),
        )
        return dict(zip(range(low, low + halves), pieces))

    def others(parts, pieces, held, c, cw):
        parts_left = [k for k in range(ep) if k not in parts]
        rows_left = [k for k in range(ep) if k not in pieces]
        results = call(
            functools.partial(rest_kernel, parts_left, rows_left, c),
            (bf16(FIELDS, part, cw),) * len(parts_left)
            + (bf16(FIELDS, part, held.shape[2]),) * len(rows_left),
            [room(cw, jnp.float32), sems(FIELDS)],
            [SMEM, VMEM, VMEM, HBM, HBM, HBM],
            (e1, send, held, w, m, v),
        )
        parts = parts | dict(zip(parts_left, results))
        pieces = pieces | dict(zip(rows_left, results[len(parts_left) :]))
        return [parts[k] for k in range(ep)], [pieces[k] for k in range(ep)]

    def split(start, width):
        return call(
            functools.partial(split_kernel, ep, start),
            (bf16(FIELDS, part, width),) * ep,
            [room(width, jnp.float32), sems(FIELDS)],
            [SMEM, HBM, HBM, HBM],
            (e1, w, m, v),
        )

    def sort(start, width):
        return call(
            functools.partial(sort_kernel, ep, start),
            (bf16(FIELDS, part, width),) * ep,
            [room(width, jnp.float32), sems(FIELDS)],
            [VMEM, HBM, HBM, HBM],
            (send, w, m, v),
        )

    def choose(pieces):
        return call(
            functools.partial(pick_kernel, ep),
            (bf16(*pieces[0].shape),) * ep,
            [],
            [SMEM] + [VMEM] * ep,
            (pick, *pieces),
        )

    def route(pieces):
        width = pieces[0].shape[2]
        return call(
            functools.partial(route_kernel, ep, dp),
            (bf16(FIELDS, block, width),) * dp,
            [room(width)],
            [SMEM, VMEM] + [VMEM] * ep,
            (part_at, send, *pieces),
        )

    def finish(*chunks):
        counts = tuple(len(pieces) for _, pieces, _ in chunks)
        widths = [pieces[0].shape[2] for _, pieces, _ in chunks]
        total = sum(counts)
        last[:] = saved
        saved[:] = [
            call(
                functools.partial(final_kernel, counts, tuple(start for _, _, start in chunks)),
                bf16(FIELDS, 1, shard, cols),
                [room(width) for width in widths for _ in range(2)] + [sems(len(chunks), FIELDS)],
                [VMEM] + [SMEM] * len(chunks) + [VMEM] * total,
                (place, *[at for at, _, _ in chunks], *[one for _, pieces, _ in chunks for one in pieces]),
                pltpu.HBM,
                **({"input_output_aliases": {1 + len(chunks) + total: 0}} if saved else {}),
            )
        ]

    def across(pieces, step):
        far = {}
        for shift in far_first(dp):
            for k in range(shift * step, shift * step + step):
                far[k] = swap(pieces[k], "dp", dp, shift)
        return [far.get(k, piece) for k, piece in enumerate(pieces)]

    saved = []
    (c, cw), (g, gw) = [(a, n) for k, a, n in chunks if k == "ep"]
    (a, aw), (b, bw) = [(a, n) for k, a, n in chunks if k == "dp"]

    c_lead, a_held, send, place = first(c, cw, a, aw)
    a_lead = lead(a_held)
    c_parts, a_parts = others(c_lead, a_lead, a_held, c, cw)
    c_parts = spread(c_parts, ep)
    a_parts = across(a_parts, halves)
    g_parts = split(g, gw)
    g_parts = spread(g_parts, ep)
    c_parts = choose(c_parts)
    c_parts = spread(c_parts, ep)
    b_parts = sort(b, bw)
    b_parts = across(b_parts, halves)
    g_parts = choose(g_parts)
    g_parts = spread(g_parts, ep)
    c_parts = route(c_parts)
    c_parts = across(c_parts, 1)
    a_parts = spread(a_parts, ep)
    g_parts = route(g_parts)
    g_parts = across(g_parts, 1)
    b_parts = spread(b_parts, ep)
    a_parts = choose(a_parts)
    a_parts = spread(a_parts, ep)
    b_parts = choose(b_parts)
    b_parts = spread(b_parts, ep)
    finish((block_at, c_parts, c))
    finish((piece_at, a_parts, a))
    finish((piece_at, b_parts, b))
    finish((block_at, g_parts, g))
    return saved[0]


def plain_destinations(bucket_offsets, writer_rank, shard_rows, groups):
    indicator = (writer_rank[:, None] == jnp.arange(groups, dtype=jnp.int32)[None, :]).astype(jnp.int32)
    before = jnp.cumsum(indicator, axis=0) - indicator
    within = jnp.sum(before * indicator, axis=1)
    return jnp.take(writer_rank * shard_rows + within, bucket_offsets)


def plain_route(stacked, target, shard_rows, groups):
    mine = lax.axis_index("dp")
    per_pair = shard_rows // groups
    table = target.reshape(groups, shard_rows)
    outgoing = jnp.argsort(lax.dynamic_index_in_dim(table, mine, 0, keepdims=False))
    sending = jnp.take(stacked, outgoing, axis=1).reshape(FIELDS, groups, per_pair, stacked.shape[2])
    arrived = lax.all_to_all(sending, "dp", split_axis=1, concat_axis=1, tiled=True)
    ordered = jnp.sort(table, axis=1)
    slots = lax.dynamic_slice_in_dim(ordered, mine * per_pair, per_pair, 1).reshape(shard_rows)
    slots = slots - mine * shard_rows
    return jnp.take(arrived.reshape(FIELDS, shard_rows, stacked.shape[2]), jnp.argsort(slots), axis=1)


def plain_on_device(w, m, v, expert_ids, bucket_offsets, writer_rank):
    groups = lax.axis_size("dp")
    shard_rows = w.shape[1]
    stacked = jnp.stack([one[0].astype(jnp.bfloat16) for one in (w, m, v)])
    target = plain_destinations(bucket_offsets, writer_rank, shard_rows, groups)
    stacked = plain_route(stacked, target, shard_rows, groups)
    pieces = lax.all_to_all(stacked[None], "ep", split_axis=2, concat_axis=0, tiled=True)
    chosen = jnp.take(pieces, jnp.argsort(expert_ids), axis=0)
    return lax.all_to_all(chosen, "ep", split_axis=0, concat_axis=2, tiled=True)[0][:, None]


def solution(mesh):
    ep, dp = mesh.shape["ep"], mesh.shape["dp"]
    specs = dict(
        mesh=mesh,
        in_specs=(P("ep", "dp", None), P("ep", "dp", None), P("ep", "dp", None), P(), P(), P()),
        out_specs=P(None, "ep", "dp", None),
        check_vma=False,
    )

    def fits(rows, cols):
        shard = rows // dp
        return (
            ep & (ep - 1) == 0
            and dp & (dp - 1) == 0
            and ep % dp == 0
            and ep >= 8
            and dp >= 4
            and shard % LANES == 0
            and shard % (16 * ep) == 0
            and cols % LANES == 0
            and rows % LANES == 0
            and cols // LANES >= sum(SHARES)
        )

    def function(w, m, v, expert_ids, bucket_offsets, writer_rank):
        rows, cols = w.shape[1:]
        args = (w, m, v, expert_ids, bucket_offsets, writer_rank)
        if not fits(rows, cols):
            return jax.shard_map(plain_on_device, **specs)(*args)
        kinds = ("ep", "ep", "dp", "dp")
        tiles = cols // LANES
        edges = [LANES * (tiles * sum(SHARES[:i]) // sum(SHARES)) for i in range(len(SHARES) + 1)]
        chunks = tuple((kind, edges[i], edges[i + 1] - edges[i]) for i, kind in enumerate(kinds))
        body = jax.shard_map(functools.partial(on_device, ep, dp, chunks), **specs)
        return body(*args)

    return function
```
